32 devices in a mesh: row: 8 (over y, x, core), col: 4 (over z).
Axes of the slice: x: 2, y: 2, z: 4, core: 2. Of those that a mesh axis runs over, the one named last changes fastest.
Arguments:
- field: float32 [64, 128, 512], P(None, 'row', 'col'), may hold values from -4 to 6.5, as said below
- conductivity: float32 [64, 128, 512], P(None, 'row', 'col'), may hold values from 35 to 5600, as said below
Outputs:
- new_field: float32 [64, 128, 512], P(None, 'row', 'col')
The draws below stay inside these ranges and needn't reach their ends.
Inputs may be any that keep to these rules, and one draw needn't show every extreme that they name: `field`: finite values. `conductivity`: positive in every cell.
All inputs are finite; a program needn't handle non-finite values.
Results may differ from the reference program's by a relative error of at most 0.0003.
Values sent between devices are 32-bit elements; how exact they have to be, the bound alone decides.
A program may use at most 64 MiB of HBM per device.

```python
import math
import jax
import jax.numpy as jnp
from jax import lax

NZ = 64
CX = 16
CY = 128
NX = 128
NY = 512


def draw_field(key, part):
    keys = jax.random.split(jax.random.fold_in(key, 23), 5)
    x_position = (jnp.arange(NX, dtype=jnp.float32) + 0.5) / NX
    y_position = (jnp.arange(NY, dtype=jnp.float32) + 0.5) / NY
    phase_x = jax.random.uniform(keys[0], (NZ, 1, 1), jnp.float32, 0.0, 2.0 * math.pi)
    phase_y = jax.random.uniform(keys[1], (NZ, 1, 1), jnp.float32, 0.0, 2.0 * math.pi)
    noise = jnp.clip(jax.random.normal(keys[2], (NZ, NX, NY), jnp.float32), -4.0, 4.0)
    offset = jax.random.uniform(keys[3], (NZ, 1, 1), jnp.float32, 0.6, 1.5)
    amplitude = 0.5
    wave_x = jnp.sin(2.0 * math.pi * x_position[None, :, None] + phase_x)
    wave_y = jnp.sin(2.0 * math.pi * y_position[None, None, :] + phase_y)
    smooth = offset + amplitude * wave_x * wave_y
    return (noise + smooth).astype(jnp.float32)


def draw_conductivity(key, part):
    keys = jax.random.split(jax.random.fold_in(key, 11), 4)
    level = jnp.exp(jax.random.uniform(keys[0], (NZ, 1, 1), jnp.float32, math.log(200.0), math.log(4000.0)))
    x_factor = jnp.exp(jax.random.uniform(keys[1], (NZ, NX // CX, 1), jnp.float32, math.log(0.5), 0.0))
    x_factor = jnp.repeat(x_factor, CX, axis=1)
    y_factor = jnp.exp(jax.random.uniform(keys[2], (NZ, 1, NY // CY), jnp.float32, math.log(0.5), 0.0))
    y_factor = jnp.repeat(y_factor, CY, axis=2)
    rough = jnp.exp(jax.random.uniform(keys[3], (NZ, NX, NY), jnp.float32, math.log(0.7), math.log(1.4)))
    return (level * x_factor * y_factor * rough).astype(jnp.float32)


def setup_inputs(seed: int = 0) -> dict:
    streams_of = jax.random.split(jax.random.key(seed), 3)
    return {
        "field": draw_field(jax.random.fold_in(streams_of[2], 71), 0),
        "conductivity": draw_conductivity(jax.random.fold_in(streams_of[2], 71), 0),
    }


z_weight = 0.02


def neighbour(values, line_axis, offset):
    length = values.shape[line_axis]
    widths = [(0, 0)] * values.ndim
    widths[line_axis] = (1, 1)
    padded = jnp.pad(values, widths)
    return lax.slice_in_dim(padded, 1 + offset, 1 + offset + length, axis=line_axis)


def diffuse(field, conductivity, line_axis, weight):
    east_face = 0.5 * weight * (conductivity + neighbour(conductivity, line_axis, 1))
    west_face = 0.5 * weight * (conductivity + neighbour(conductivity, line_axis, -1))
    flux_here = east_face * (neighbour(field, line_axis, 1) - field) - west_face * (field - neighbour(field, line_axis, -1))
    return flux_here, west_face, east_face


def thomas(below_diag, above_diag, right_side):
    diagonal = 1.0 - below_diag - above_diag

    def forward(state_now, inputs):
        ratio_prev, value_prev = state_now
        below_here, diag_here, above_here, source_here = inputs
        pivot_here = diag_here - below_here * ratio_prev
        ratio_here = above_here / pivot_here
        value_here = (source_here - below_here * value_prev) / pivot_here
        return (ratio_here, value_here), (ratio_here, value_here)

    zero_plane = jnp.zeros_like(right_side[0])
    unused, outputs = lax.scan(forward, (zero_plane, zero_plane), (below_diag, diagonal, above_diag, right_side))

    def backward(next_value, inputs):
        ratio_here, value_here = inputs
        solved = value_here - ratio_here * next_value
        return solved, solved

    unused_last, solution = lax.scan(backward, zero_plane, outputs, reverse=True)
    return solution


def solve_lines(below_diag, above_diag, right_side, line_axis):
    solution = thomas(jnp.moveaxis(below_diag, line_axis, 0), jnp.moveaxis(above_diag, line_axis, 0), jnp.moveaxis(right_side, line_axis, 0))
    return jnp.moveaxis(solution, 0, line_axis)


def reference(field, conductivity):
    flux_zdir, west_zdir, east_zdir = diffuse(field, conductivity, 0, z_weight)
    flux_xdir, west_xdir, east_xdir = diffuse(field, conductivity, 1, 1.0)
    flux_ydir, west_ydir, east_ydir = diffuse(field, conductivity, 2, 1.0)
    explicit = flux_xdir + flux_ydir + flux_zdir
    delta_xdir = solve_lines(-west_xdir, -east_xdir, explicit, 1)
    delta_ydir = solve_lines(-west_ydir, -east_ydir, delta_xdir, 2)
    return field + delta_ydir
```

```python
import functools

import jax
import jax.numpy as jnp
from jax import lax
from jax.experimental import pallas as pl
from jax.experimental.pallas import tpu as pltpu
from jax.sharding import PartitionSpec as P

MESH = pl.DeviceIdType.MESH
z_weight = 0.02
LANES = 128
UNROLL = 8


def send_all(axis, count, source_of, target, send_sems, recv_sems):
    me = lax.axis_index(axis)
    copies = []
    for step in range(1, count):
        peer = lax.rem(me + step, count)
        copy = pltpu.make_async_remote_copy(
            src_ref=source_of(peer),
            dst_ref=target.at[me],
            send_sem=send_sems.at[step],
            recv_sem=recv_sems.at[step],
            device_id={axis: peer},
            device_id_type=MESH,
        )
        copy.start()
        copies.append(copy)
    return copies


def factor_faces(mats, count):
    rows = []
    h_prev = None
    for m in range(count - 1):
        face = 0.5 * (mats(m, 4) + mats(m + 1, 3))
        pivot = 1.0 / face + mats(m + 1, 0) + mats(m, 2)
        if m > 0:
            pivot = pivot - mats(m, 1) * h_prev
        inverse = 1.0 / pivot
        h_prev = mats(m + 1, 1) * inverse
        rows.append((inverse, h_prev))
    return rows


def solve_faces(rows, mats, values, count):
    partial = []
    for m in range(count - 1):
        right = values(m + 1, 0) - values(m, 1)
        if m > 0:
            right = right + mats(m, 1) * partial[-1]
        partial.append(right * rows[m][0])
    fluxes = [None] * (count - 1)
    for m in reversed(range(count - 1)):
        fluxes[m] = partial[m]
        if m < count - 2:
            fluxes[m] = fluxes[m] + rows[m][1] * fluxes[m + 1]
    return fluxes


def kernel(
    dims, field_hbm, cond_hbm, out_ref,
    fbuf, cbuf, xu, xk, xr, xinv, xw, xb, kt, yr, yinv, yw, dt,
    pack, pack_l, pack_r, xm, xm_in, xv, xv_in, xj, xj_in, ym_in, yv_in, ym, yv,
    in_sems, halo_send, halo_recv, xm_send, xm_recv, xv_send, xv_recv, xj_send, xj_recv,
    ym_send, ym_recv, yv_send, yv_recv,
):
    n_row, n_col, nz, nx, ny = dims
    zs = nz // n_row
    blocks = nz * nx // LANES
    row = lax.axis_index("row")
    col = lax.axis_index("col")
    load_c = pltpu.make_async_copy(cond_hbm, cbuf.at[pl.ds(nx, nz * nx)], in_sems.at[0])
    load_f = pltpu.make_async_copy(field_hbm, fbuf.at[pl.ds(nx, nz * nx)], in_sems.at[1])
    load_c.start()
    load_f.start()
    barrier = pltpu.get_barrier_semaphore()
    for step in range(1, n_row):
        pl.semaphore_signal(
            barrier, inc=1, device_id={"row": lax.rem(row + step, n_row)}, device_id_type=MESH
        )
    for step in range(1, n_col):
        pl.semaphore_signal(
            barrier, inc=1, device_id={"col": lax.rem(col + step, n_col)}, device_id_type=MESH
        )
    edge = jnp.zeros((nx, ny), jnp.float32)
    for buf in (fbuf, cbuf):
        buf[pl.ds(0, nx), :] = edge
        buf[pl.ds((nz + 1) * nx, nx), :] = edge

    @pl.when(col == 0)
    def _():
        pack_l[...] = jnp.zeros_like(pack_l)

    @pl.when(col == n_col - 1)
    def _():
        pack_r[...] = jnp.zeros_like(pack_r)

    load_c.wait()
    load_f.wait()

    lane = lax.broadcasted_iota(jnp.int32, (nz, ny), 1)
    pair = lane // 2
    packed = jnp.zeros((nz, ny), jnp.float32)
    for x in range(nx):
        u = fbuf[pl.ds(nx + x, nz, stride=nx), :]
        k = cbuf[pl.ds(nx + x, nz, stride=nx), :]
        xu[x] = u
        xk[x] = k
        packed = jnp.where(pair == x, pltpu.roll(u, 2 * x + 1, 1), packed)
        packed = jnp.where(pair == nx + x, pltpu.roll(k, 2 * (nx + x) + 1, 1), packed)
    pack[...] = packed
    pl.semaphore_wait(barrier, n_row + n_col - 2)

    to_right = pltpu.make_async_remote_copy(
        src_ref=pack, dst_ref=pack_l, send_sem=halo_send.at[0], recv_sem=halo_recv.at[0],
        device_id={"col": jnp.minimum(col + 1, n_col - 1)}, device_id_type=MESH,
    )
    to_left = pltpu.make_async_remote_copy(
        src_ref=pack, dst_ref=pack_r, send_sem=halo_send.at[1], recv_sem=halo_recv.at[1],
        device_id={"col": jnp.maximum(col - 1, 0)}, device_id_type=MESH,
    )

    @pl.when(col < n_col - 1)
    def _():
        to_right.start()

    @pl.when(col > 0)
    def _():
        to_left.start()

    first_x = jnp.where(row == 0, 0.5, 0.0).astype(jnp.float32)
    last_x = jnp.where(row == n_row - 1, 0.5, 0.0).astype(jnp.float32)
    first_y = jnp.where(col == 0, 0.5, 0.0).astype(jnp.float32)
    last_y = jnp.where(col == n_col - 1, 0.5, 0.0).astype(jnp.float32)
    s = 1.0 + first_x * xk[0]
    prod = jnp.ones((nz, ny), jnp.float32)
    gff = jnp.zeros((nz, ny), jnp.float32)
    for x in range(nx):
        if x < nx - 1:
            e = 0.5 * (xk[x] + xk[x + 1])
            inv = 1.0 / (s + e)
            ratio = e * inv
            xr[x] = ratio
        else:
            inv = 1.0 / (s + last_x * xk[x])
        weight = prod * inv
        xinv[x] = inv
        xw[x] = weight
        gff = gff + prod * weight
        if x < nx - 1:
            prod = prod * ratio
            s = 1.0 + s * ratio
    for q, value in enumerate((gff, weight, inv, xk[0], xk[nx - 1])):
        for j in range(n_row):
            xm[j, q] = value[j * zs : (j + 1) * zs]
    xm_copies = send_all("row", n_row, lambda peer: xm.at[peer], xm_in, xm_send, xm_recv)
    xm_in[row] = xm[row]

    below = first_x * xk[0] * xu[0]
    for x in range(nx):
        u = xu[x]
        k = xk[x]
        flux = 0.5 * (k + pltpu.roll(k, ny - 1, 1)) * (pltpu.roll(u, ny - 1, 1) - u)
        flux = jnp.where(lane == ny - 1, 0.0, flux)
        total = flux - pltpu.roll(flux, 1, 1)
        k_up = cbuf[pl.ds(2 * nx + x, nz, stride=nx), :]
        u_up = fbuf[pl.ds(2 * nx + x, nz, stride=nx), :]
        k_down = cbuf[pl.ds(x, nz, stride=nx), :]
        u_down = fbuf[pl.ds(x, nz, stride=nx), :]
        total = total + 0.5 * z_weight * ((k + k_up) * (u_up - u) - (k + k_down) * (u - u_down))
        if x < nx - 1:
            above = 0.5 * (k + xk[x + 1]) * (xu[x + 1] - u)
        else:
            above = -last_x * k * u
        xb[x] = total + (above - below)
        below = above

    for p in range(blocks):
        per = LANES // nz
        tile = jnp.concatenate([xk[p * per + i] for i in range(per)], axis=0)
        kt[pl.ds(p, ny, stride=blocks), :] = tile.T

    @pl.when(col > 0)
    def _():
        to_right.wait_recv()

    @pl.when(col < n_col - 1)
    def _():
        to_left.wait_recv()

    other = jnp.where(
        lane % 2 == 0, pltpu.roll(pack_r[...], ny - 1, 1), pltpu.roll(pack_l[...], 1, 1)
    )
    mine = pack[...]
    k_sum = pltpu.roll(mine + other, ny - 2 * nx, 1)
    outer = 0.5 * k_sum * (other - mine)
    ends = (lane == 0) | (lane == ny - 1)

    value = None
    for x in range(nx):
        here = xb[x] + jnp.where(ends, pltpu.roll(outer, ny - 1 - 2 * x, 1), 0.0)
        value = here if x == 0 else here + xr[x - 1] * value
        xb[x] = value
        free_first = xw[x] * value if x == 0 else free_first + xw[x] * value
    free_last = xinv[nx - 1] * value
    for q, v in enumerate((xu[0] + free_first, xu[nx - 1] + free_last)):
        for j in range(n_row):
            xv[j, q] = v[j * zs : (j + 1) * zs]
    xv_copies = send_all("row", n_row, lambda peer: xv.at[peer], xv_in, xv_send, xv_recv)
    xv_in[row] = xv[row]

    def y_at(y):
        if isinstance(y, int):
            return pl.ds(y * blocks, blocks)
        return pl.ds(pl.multiple_of(y * blocks, blocks), blocks)

    def y_factor(y, state):
        k, s, prod, gff = state
        k_next = kt[y_at(y + 1), :]
        e = 0.5 * (k + k_next)
        inv = 1.0 / (s + e)
        ratio = e * inv
        weight = prod * inv
        yr[y_at(y), :] = ratio
        yinv[y_at(y), :] = inv
        yw[y_at(y), :] = weight
        return k_next, 1.0 + s * ratio, prod * ratio, gff + prod * weight

    def unrolled(step, base, state):
        for i in range(UNROLL):
            state = step(base * UNROLL + i, state)
        return state

    trips = ny // UNROLL
    k_first = kt[y_at(0), :]
    one = jnp.ones_like(k_first)
    state = (k_first, 1.0 + first_y * k_first, one, jnp.zeros_like(one))
    state = lax.fori_loop(0, trips - 1, lambda t, c: unrolled(y_factor, t, c), state)
    for y in range((trips - 1) * UNROLL, ny - 1):
        state = y_factor(y, state)
    k_last, s, prod, gff = state
    inv = 1.0 / (s + last_y * k_last)
    weight = prod * inv
    gff = gff + prod * weight
    yinv[y_at(ny - 1), :] = inv
    yw[y_at(ny - 1), :] = weight
    for q, v in enumerate((gff, weight, inv, k_first, k_last)):
        ym[q] = v
    ym_copies = send_all("col", n_col, lambda peer: ym, ym_in, ym_send, ym_recv)
    ym_in[col] = ym[...]

    for copy in xm_copies:
        copy.wait_recv()
    x_mats = lambda m, q: xm_in[m, q]
    x_rows = factor_faces(x_mats, n_row)
    for copy in xv_copies:
        copy.wait_recv()
    fluxes = solve_faces(x_rows, x_mats, lambda m, q: xv_in[m, q], n_row)
    nothing = jnp.zeros((zs, ny), jnp.float32)
    for m in range(n_row):
        xj[m, 0] = fluxes[m - 1] if m > 0 else nothing
        xj[m, 1] = fluxes[m] if m < n_row - 1 else nothing
    xj_copies = send_all("row", n_row, lambda peer: xj.at[peer], xj_in, xj_send, xj_recv)
    xj_in[row] = xj[row]

    for copy in ym_copies:
        copy.wait_recv()
    y_mats = lambda m, q: ym_in[m, q]
    y_rows = factor_faces(y_mats, n_col)
    for copy in xj_copies:
        copy.wait_recv()

    enter = jnp.concatenate([xj_in[j, 0] for j in range(n_row)], axis=0)
    leave = jnp.concatenate([xj_in[j, 1] for j in range(n_row)], axis=0)
    for x in reversed(range(nx)):
        if x == nx - 1:
            delta = (xb[x] + leave) * xinv[x] - enter * xw[x]
        else:
            delta = xb[x] * xinv[x] - enter * xw[x] + xr[x] * delta
        xb[x] = delta
    for p in range(blocks):
        tile = jnp.concatenate([xb[p * per + i] for i in range(per)], axis=0)
        dt[pl.ds(p, ny, stride=blocks), :] = tile.T

    def y_forward(y, state):
        value, free_first = state
        value = dt[y_at(y), :] + yr[y_at(y - 1), :] * value
        dt[y_at(y), :] = value
        return value, free_first + yw[y_at(y), :] * value

    value = dt[y_at(0), :]
    state = (value, yw[y_at(0), :] * value)
    for y in range(1, UNROLL):
        state = y_forward(y, state)
    value, free_first = lax.fori_loop(1, trips, lambda t, c: unrolled(y_forward, t, c), state)
    yv[0] = free_first
    yv[1] = yinv[y_at(ny - 1), :] * value
    yv_copies = send_all("col", n_col, lambda peer: yv, yv_in, yv_send, yv_recv)
    yv_in[col] = yv[...]
    for copy in yv_copies:
        copy.wait_recv()
    fluxes = solve_faces(y_rows, y_mats, lambda m, q: yv_in[m, q], n_col)
    enter = jnp.zeros_like(one)
    leave = jnp.zeros_like(one)
    for m in range(n_col - 1):
        enter = jnp.where(col == m + 1, fluxes[m], enter)
        leave = jnp.where(col == m, fluxes[m], leave)

    def y_backward(y, delta):
        free = dt[y_at(y), :] * yinv[y_at(y), :] - enter * yw[y_at(y), :]
        delta = free + yr[y_at(y), :] * delta
        dt[y_at(y), :] = delta
        return delta

    def y_backward_trip(t, delta):
        top = ny - 1 - t * UNROLL
        for i in range(UNROLL):
            delta = y_backward(top - i, delta)
        return delta

    delta = (value + leave) * yinv[y_at(ny - 1), :] - enter * yw[y_at(ny - 1), :]
    dt[y_at(ny - 1), :] = delta
    for y in reversed(range(ny - UNROLL, ny - 1)):
        delta = y_backward(y, delta)
    lax.fori_loop(1, trips, y_backward_trip, delta)
    for p in range(blocks):
        tile = dt[pl.ds(p, ny, stride=blocks), :].T
        for i in range(per):
            x = p * per + i
            out_ref[pl.ds(x, nz, stride=nx), :] = tile[i * nz : (i + 1) * nz]

    @pl.when(col < n_col - 1)
    def _():
        to_right.wait_send()

    @pl.when(col > 0)
    def _():
        to_left.wait_send()

    for copies in (xm_copies, xv_copies, xj_copies, ym_copies, yv_copies):
        for copy in copies:
            copy.wait_send()


def solution(mesh):
    n_row, n_col = mesh.shape["row"], mesh.shape["col"]

    def on_device(field, conductivity):
        nz, nx, ny = field.shape
        zs = nz // n_row
        blocks = nz * nx // LANES
        flat = (nz * nx, ny)
        tall = pltpu.VMEM(((nz + 2) * nx, ny), jnp.float32)
        cube = pltpu.VMEM((nx, nz, ny), jnp.float32)
        lines = pltpu.VMEM((ny * blocks, LANES), jnp.float32)
        plane = pltpu.VMEM((nz, ny), jnp.float32)
        part = lambda count: pltpu.VMEM((n_row, count, zs, ny), jnp.float32)
        whole = lambda *lead: pltpu.VMEM((*lead, blocks, LANES), jnp.float32)
        sems = lambda count: pltpu.SemaphoreType.DMA((count,))
        delta = pl.pallas_call(
            functools.partial(kernel, (n_row, n_col, nz, nx, ny)),
            out_shape=jax.ShapeDtypeStruct(flat, jnp.float32),
            in_specs=[pl.BlockSpec(memory_space=pl.ANY)] * 2,
            out_specs=pl.BlockSpec(memory_space=pltpu.VMEM),
            scratch_shapes=[
                tall, tall, cube, cube, cube, cube, cube, cube,
                lines, lines, lines, lines, lines,
                plane, plane, plane,
                part(5), part(5), part(2), part(2), part(2), part(2),
                whole(n_col, 5), whole(n_col, 2), whole(5), whole(2),
                sems(2), sems(2), sems(2),
                *[sems(n_row)] * 6,
                *[sems(n_col)] * 4,
            ],
            compiler_params=pltpu.CompilerParams(
                collective_id=0, has_side_effects=True, vmem_limit_bytes=32 * 1024 * 1024
            ),
            name="adi_step",
        )(field.reshape(flat), conductivity.reshape(flat))
        return field + delta.reshape(field.shape)

    spec = P(None, "row", "col")
    return jax.shard_map(
        on_device, mesh=mesh, in_specs=(spec, spec), out_specs=spec, check_vma=False
    )
```

```python
import functools

import jax
import jax.numpy as jnp
from jax import lax
from jax.experimental import pallas as pl
from jax.experimental.pallas import tpu as pltpu
from jax.sharding import PartitionSpec as P

MESH = pl.DeviceIdType.MESH
z_weight = 0.02
LANES = 128
UNROLL = 8
PAD = 8


def send_all(axis, count, source_of, target, send_sems, recv_sems):
    me = lax.axis_index(axis)
    copies = []
    for step in range(1, count):
        peer = lax.rem(me + step, count)
        copy = pltpu.make_async_remote_copy(
            src_ref=source_of(peer),
            dst_ref=target.at[me],
            send_sem=send_sems.at[step],
            recv_sem=recv_sems.at[step],
            device_id={axis: peer},
            device_id_type=MESH,
        )
        copy.start()
        copies.append(copy)
    return copies


def factor_faces(mats, count):
    rows = []
    h_prev = None
    for m in range(count - 1):
        face = 0.5 * (mats(m, 4) + mats(m + 1, 3))
        pivot = 1.0 / face + mats(m + 1, 0) + mats(m, 2)
        if m > 0:
            pivot = pivot - mats(m, 1) * h_prev
        inverse = 1.0 / pivot
        h_prev = mats(m + 1, 1) * inverse
        rows.append((inverse, h_prev))
    return rows


def solve_faces(rows, mats, values, count):
    partial = []
    for m in range(count - 1):
        right = values(m + 1, 0) - values(m, 1)
        if m > 0:
            right = right + mats(m, 1) * partial[-1]
        partial.append(right * rows[m][0])
    fluxes = [None] * (count - 1)
    for m in reversed(range(count - 1)):
        fluxes[m] = partial[m]
        if m < count - 2:
            fluxes[m] = fluxes[m] + rows[m][1] * fluxes[m + 1]
    return fluxes


def kernel(
    dims, field_hbm, cond_hbm, out_ref,
    xu, xk, xr, xinv, xw, xb, kt, yr, yinv, yw, dt,
    pack, pack_l, pack_r, xm, xm_in, xv, xv_in, xj, xj_in, ym_in, yv_in, ym, yv,
    in_sems, halo_send, halo_recv, xm_send, xm_recv, xv_send, xv_recv, xj_send, xj_recv,
    ym_send, ym_recv, yv_send, yv_recv,
):
    n_row, n_col, nz, nx, ny = dims
    zs = nz // n_row
    blocks = nz * nx // LANES
    row = lax.axis_index("row")
    col = lax.axis_index("col")
    inner = pl.ds(PAD, nz)
    loads = []
    for x in range(nx):
        for source, target, sem in ((cond_hbm, xk, 0), (field_hbm, xu, 1)):
            load = pltpu.make_async_copy(
                source.at[:, x, 0, :], target.at[x, inner, :], in_sems.at[sem, x]
            )
            load.start()
            loads.append(load)
    barrier = pltpu.get_barrier_semaphore()
    for step in range(1, n_row):
        pl.semaphore_signal(
            barrier, inc=1, device_id={"row": lax.rem(row + step, n_row)}, device_id_type=MESH
        )
    for step in range(1, n_col):
        pl.semaphore_signal(
            barrier, inc=1, device_id={"col": lax.rem(col + step, n_col)}, device_id_type=MESH
        )
    edge = jnp.zeros((nx, PAD, ny), jnp.float32)
    for buf in (xu, xk):
        buf[:, pl.ds(0, PAD), :] = edge
        buf[:, pl.ds(PAD + nz, PAD), :] = edge
    field = lambda x: xu[x, inner, :]
    cond = lambda x: xk[x, inner, :]

    @pl.when(col == 0)
    def _():
        pack_l[...] = jnp.zeros_like(pack_l)

    @pl.when(col == n_col - 1)
    def _():
        pack_r[...] = jnp.zeros_like(pack_r)

    lane = lax.broadcasted_iota(jnp.int32, (nz, ny), 1)
    pair = lane // 2
    packed = jnp.zeros((nz, ny), jnp.float32)
    for x in range(nx):
        loads[2 * x].wait()
        loads[2 * x + 1].wait()
        u, k = field(x), cond(x)
        packed = jnp.where(pair == x, pltpu.roll(u, 2 * x + 1, 1), packed)
        packed = jnp.where(pair == nx + x, pltpu.roll(k, 2 * (nx + x) + 1, 1), packed)
    pack[...] = packed
    pl.semaphore_wait(barrier, n_row + n_col - 2)

    to_right = pltpu.make_async_remote_copy(
        src_ref=pack, dst_ref=pack_l, send_sem=halo_send.at[0], recv_sem=halo_recv.at[0],
        device_id={"col": jnp.minimum(col + 1, n_col - 1)}, device_id_type=MESH,
    )
    to_left = pltpu.make_async_remote_copy(
        src_ref=pack, dst_ref=pack_r, send_sem=halo_send.at[1], recv_sem=halo_recv.at[1],
        device_id={"col": jnp.maximum(col - 1, 0)}, device_id_type=MESH,
    )

    @pl.when(col < n_col - 1)
    def _():
        to_right.start()

    @pl.when(col > 0)
    def _():
        to_left.start()

    first_x = jnp.where(row == 0, 0.5, 0.0).astype(jnp.float32)
    last_x = jnp.where(row == n_row - 1, 0.5, 0.0).astype(jnp.float32)
    first_y = jnp.where(col == 0, 0.5, 0.0).astype(jnp.float32)
    last_y = jnp.where(col == n_col - 1, 0.5, 0.0).astype(jnp.float32)
    s = 1.0 + first_x * cond(0)
    prod = jnp.ones((nz, ny), jnp.float32)
    gff = jnp.zeros((nz, ny), jnp.float32)
    for x in range(nx):
        if x < nx - 1:
            e = 0.5 * (cond(x) + cond(x + 1))
            inv = 1.0 / (s + e)
            ratio = e * inv
            xr[x] = ratio
        else:
            inv = 1.0 / (s + last_x * cond(x))
        weight = prod * inv
        xinv[x] = inv
        xw[x] = weight
        gff = gff + prod * weight
        if x < nx - 1:
            prod = prod * ratio
            s = 1.0 + s * ratio
    for q, value in enumerate((gff, weight, inv, cond(0), cond(nx - 1))):
        for j in range(n_row):
            xm[j, q] = value[j * zs : (j + 1) * zs]
    xm_copies = send_all("row", n_row, lambda peer: xm.at[peer], xm_in, xm_send, xm_recv)
    xm_in[row] = xm[row]

    below = first_x * cond(0) * field(0)
    for x in range(nx):
        u = field(x)
        k = cond(x)
        flux = 0.5 * (k + pltpu.roll(k, ny - 1, 1)) * (pltpu.roll(u, ny - 1, 1) - u)
        flux = jnp.where(lane == ny - 1, 0.0, flux)
        total = flux - pltpu.roll(flux, 1, 1)
        k_up, u_up = xk[x, pl.ds(PAD + 1, nz), :], xu[x, pl.ds(PAD + 1, nz), :]
        k_down, u_down = xk[x, pl.ds(PAD - 1, nz), :], xu[x, pl.ds(PAD - 1, nz), :]
        total = total + 0.5 * z_weight * ((k + k_up) * (u_up - u) - (k + k_down) * (u - u_down))
        if x < nx - 1:
            above = 0.5 * (k + cond(x + 1)) * (field(x + 1) - u)
        else:
            above = -last_x * k * u
        xb[x] = total + (above - below)
        below = above

    for p in range(blocks):
        per = LANES // nz
        tile = jnp.concatenate([cond(p * per + i) for i in range(per)], axis=0)
        kt[pl.ds(p, ny, stride=blocks), :] = tile.T

    @pl.when(col > 0)
    def _():
        to_right.wait_recv()

    @pl.when(col < n_col - 1)
    def _():
        to_left.wait_recv()

    other = jnp.where(
        lane % 2 == 0, pltpu.roll(pack_r[...], ny - 1, 1), pltpu.roll(pack_l[...], 1, 1)
    )
    mine = pack[...]
    k_sum = pltpu.roll(mine + other, ny - 2 * nx, 1)
    outer = 0.5 * k_sum * (other - mine)
    ends = (lane == 0) | (lane == ny - 1)

    value = None
    for x in range(nx):
        here = xb[x] + jnp.where(ends, pltpu.roll(outer, ny - 1 - 2 * x, 1), 0.0)
        value = here if x == 0 else here + xr[x - 1] * value
        xb[x] = value
        free_first = xw[x] * value if x == 0 else free_first + xw[x] * value
    free_last = xinv[nx - 1] * value
    for q, v in enumerate((field(0) + free_first, field(nx - 1) + free_last)):
        for j in range(n_row):
            xv[j, q] = v[j * zs : (j + 1) * zs]
    xv_copies = send_all("row", n_row, lambda peer: xv.at[peer], xv_in, xv_send, xv_recv)
    xv_in[row] = xv[row]

    def y_at(y):
        if isinstance(y, int):
            return pl.ds(y * blocks, blocks)
        return pl.ds(pl.multiple_of(y * blocks, blocks), blocks)

    def y_factor(y, state):
        k, s, prod, gff = state
        k_next = kt[y_at(y + 1), :]
        e = 0.5 * (k + k_next)
        inv = 1.0 / (s + e)
        ratio = e * inv
        weight = prod * inv
        yr[y_at(y), :] = ratio
        yinv[y_at(y), :] = inv
        yw[y_at(y), :] = weight
        return k_next, 1.0 + s * ratio, prod * ratio, gff + prod * weight

    def unrolled(step, base, state):
        for i in range(UNROLL):
            state = step(base * UNROLL + i, state)
        return state

    trips = ny // UNROLL
    k_first = kt[y_at(0), :]
    one = jnp.ones_like(k_first)
    state = (k_first, 1.0 + first_y * k_first, one, jnp.zeros_like(one))
    state = lax.fori_loop(0, trips - 1, lambda t, c: unrolled(y_factor, t, c), state)
    for y in range((trips - 1) * UNROLL, ny - 1):
        state = y_factor(y, state)
    k_last, s, prod, gff = state
    inv = 1.0 / (s + last_y * k_last)
    weight = prod * inv
    gff = gff + prod * weight
    yinv[y_at(ny - 1), :] = inv
    yw[y_at(ny - 1), :] = weight
    for q, v in enumerate((gff, weight, inv, k_first, k_last)):
        ym[q] = v
    ym_copies = send_all("col", n_col, lambda peer: ym, ym_in, ym_send, ym_recv)
    ym_in[col] = ym[...]

    for copy in xm_copies:
        copy.wait_recv()
    x_mats = lambda m, q: xm_in[m, q]
    x_rows = factor_faces(x_mats, n_row)
    for copy in xv_copies:
        copy.wait_recv()
    fluxes = solve_faces(x_rows, x_mats, lambda m, q: xv_in[m, q], n_row)
    nothing = jnp.zeros((zs, ny), jnp.float32)
    for m in range(n_row):
        xj[m, 0] = fluxes[m - 1] if m > 0 else nothing
        xj[m, 1] = fluxes[m] if m < n_row - 1 else nothing
    xj_copies = send_all("row", n_row, lambda peer: xj.at[peer], xj_in, xj_send, xj_recv)
    xj_in[row] = xj[row]

    for copy in ym_copies:
        copy.wait_recv()
    y_mats = lambda m, q: ym_in[m, q]
    y_rows = factor_faces(y_mats, n_col)
    for copy in xj_copies:
        copy.wait_recv()

    enter = jnp.concatenate([xj_in[j, 0] for j in range(n_row)], axis=0)
    leave = jnp.concatenate([xj_in[j, 1] for j in range(n_row)], axis=0)
    for x in reversed(range(nx)):
        if x == nx - 1:
            delta = (xb[x] + leave) * xinv[x] - enter * xw[x]
        else:
            delta = xb[x] * xinv[x] - enter * xw[x] + xr[x] * delta
        xb[x] = delta
    for p in range(blocks):
        tile = jnp.concatenate([xb[p * per + i] for i in range(per)], axis=0)
        dt[pl.ds(p, ny, stride=blocks), :] = tile.T

    def y_forward(y, state):
        value, free_first = state
        value = dt[y_at(y), :] + yr[y_at(y - 1), :] * value
        dt[y_at(y), :] = value
        return value, free_first + yw[y_at(y), :] * value

    value = dt[y_at(0), :]
    state = (value, yw[y_at(0), :] * value)
    for y in range(1, UNROLL):
        state = y_forward(y, state)
    value, free_first = lax.fori_loop(1, trips, lambda t, c: unrolled(y_forward, t, c), state)
    yv[0] = free_first
    yv[1] = yinv[y_at(ny - 1), :] * value
    yv_copies = send_all("col", n_col, lambda peer: yv, yv_in, yv_send, yv_recv)
    yv_in[col] = yv[...]
    for copy in yv_copies:
        copy.wait_recv()
    fluxes = solve_faces(y_rows, y_mats, lambda m, q: yv_in[m, q], n_col)
    enter = jnp.zeros_like(one)
    leave = jnp.zeros_like(one)
    for m in range(n_col - 1):
        enter = jnp.where(col == m + 1, fluxes[m], enter)
        leave = jnp.where(col == m, fluxes[m], leave)

    def y_backward(y, delta):
        free = dt[y_at(y), :] * yinv[y_at(y), :] - enter * yw[y_at(y), :]
        delta = free + yr[y_at(y), :] * delta
        dt[y_at(y), :] = delta
        return delta

    def y_backward_trip(t, delta):
        top = ny - 1 - t * UNROLL
        for i in range(UNROLL):
            delta = y_backward(top - i, delta)
        return delta

    delta = (value + leave) * yinv[y_at(ny - 1), :] - enter * yw[y_at(ny - 1), :]
    dt[y_at(ny - 1), :] = delta
    for y in reversed(range(ny - UNROLL, ny - 1)):
        delta = y_backward(y, delta)
    lax.fori_loop(1, trips, y_backward_trip, delta)
    for p in range(blocks):
        tile = dt[pl.ds(p, ny, stride=blocks), :].T
        for i in range(per):
            x = p * per + i
            out_ref[pl.ds(x, nz, stride=nx), :] = field(x) + tile[i * nz : (i + 1) * nz]

    @pl.when(col < n_col - 1)
    def _():
        to_right.wait_send()

    @pl.when(col > 0)
    def _():
        to_left.wait_send()

    for copies in (xm_copies, xv_copies, xj_copies, ym_copies, yv_copies):
        for copy in copies:
            copy.wait_send()


def solution(mesh):
    n_row, n_col = mesh.shape["row"], mesh.shape["col"]

    def on_device(field, conductivity):
        nz, nx, ny = field.shape
        zs = nz // n_row
        blocks = nz * nx // LANES
        flat = (nz * nx, ny)
        tall = pltpu.VMEM((nx, nz + 2 * PAD, ny), jnp.float32)
        cube = pltpu.VMEM((nx, nz, ny), jnp.float32)
        lines = pltpu.VMEM((ny * blocks, LANES), jnp.float32)
        plane = pltpu.VMEM((nz, ny), jnp.float32)
        part = lambda count: pltpu.VMEM((n_row, count, zs, ny), jnp.float32)
        whole = lambda *lead: pltpu.VMEM((*lead, blocks, LANES), jnp.float32)
        sems = lambda count: pltpu.SemaphoreType.DMA((count,))
        rows = (nz, nx, 1, ny)
        out = pl.pallas_call(
            functools.partial(kernel, (n_row, n_col, nz, nx, ny)),
            out_shape=jax.ShapeDtypeStruct(flat, jnp.float32),
            in_specs=[pl.BlockSpec(memory_space=pltpu.HBM)] * 2,
            out_specs=pl.BlockSpec(memory_space=pltpu.VMEM),
            scratch_shapes=[
                tall, tall, cube, cube, cube, cube,
                lines, lines, lines, lines, lines,
                plane, plane, plane,
                part(5), part(5), part(2), part(2), part(2), part(2),
                whole(n_col, 5), whole(n_col, 2), whole(5), whole(2),
                pltpu.SemaphoreType.DMA((2, nx)), sems(2), sems(2),
                *[sems(n_row)] * 6,
                *[sems(n_col)] * 4,
            ],
            compiler_params=pltpu.CompilerParams(
                collective_id=0, has_side_effects=True, vmem_limit_bytes=32 * 1024 * 1024
            ),
            name="adi_step",
        )(
            pltpu.with_memory_space_constraint(field.reshape(rows), pltpu.HBM),
            pltpu.with_memory_space_constraint(conductivity.reshape(rows), pltpu.HBM),
        )
        return out.reshape(field.shape)

    spec = P(None, "row", "col")
    return jax.shard_map(
        on_device, mesh=mesh, in_specs=(spec, spec), out_specs=spec, check_vma=False
    )
```

```python
import functools

import jax
import jax.numpy as jnp
from jax import lax
from jax.experimental import pallas as pl
from jax.experimental.pallas import tpu as pltpu
from jax.sharding import PartitionSpec as P

MESH = pl.DeviceIdType.MESH
z_weight = 0.02
LANES = 128
UNROLL = 8
PAD = 8
PITCH_PAD = 8


def row_groups(count):
    every = range(1, count)
    if count < 8 or count & (count - 1):
        return list(every), False
    return [o for o in every if not (o & 2 and o >> 2)], True


def flipped(index, offset, count):
    if count & (count - 1):
        return lax.rem(index + offset, count)
    result = index
    bit = 1
    while bit <= offset:
        if offset & bit:
            result = result + bit * (1 - 2 * ((index // bit) % 2))
        bit *= 2
    return result


def send_all(axis, count, source_of, target, send_sems, recv_sems):
    me = lax.axis_index(axis)
    copies = []
    for step in range(1, count):
        peer = lax.rem(me + step, count)
        copy = pltpu.make_async_remote_copy(
            src_ref=source_of(peer),
            dst_ref=target.at[me],
            send_sem=send_sems.at[step],
            recv_sem=recv_sems.at[step],
            device_id={axis: peer},
            device_id_type=MESH,
        )
        copy.start()
        copies.append(copy)
    return copies


def factor_faces(mats, count):
    rows = []
    h_prev = None
    for m in range(count - 1):
        face = 0.5 * (mats(m, 4) + mats(m + 1, 3))
        pivot = 1.0 / face + mats(m + 1, 0) + mats(m, 2)
        if m > 0:
            pivot = pivot - mats(m, 1) * h_prev
        inverse = 1.0 / pivot
        h_prev = mats(m + 1, 1) * inverse
        rows.append((inverse, h_prev))
    return rows


def solve_faces(rows, mats, values, count):
    partial = []
    for m in range(count - 1):
        right = values(m + 1, 0) - values(m, 1)
        if m > 0:
            right = right + mats(m, 1) * partial[-1]
        partial.append(right * rows[m][0])
    fluxes = [None] * (count - 1)
    for m in reversed(range(count - 1)):
        fluxes[m] = partial[m]
        if m < count - 2:
            fluxes[m] = fluxes[m] + rows[m][1] * fluxes[m + 1]
    return fluxes


def kernel(
    dims, field_hbm, cond_hbm, out_ref,
    zu, zk, xu, xk, xr, xinv, xw, xb, kt, yr, yinv, yw, dt,
    pack, pack_l, pack_r, xm, xm_in, xv, xv_in, xj, xj_in, ym_in, yv_in, ym, yv,
    in_sems, halo_send, halo_recv, xm_send, xm_recv, xv_send, xv_recv, xj_send, xj_recv,
    ym_send, ym_recv, yv_send, yv_recv, row_token, col_token,
):
    n_row, n_col, nz, nx, ny = dims
    zs = nz // n_row
    blocks = nz * nx // LANES
    row = lax.axis_index("row")
    col = lax.axis_index("col")
    inner = pl.ds(PAD, nz)
    loads = []
    for source, target, sem in ((field_hbm, zu, 0), (cond_hbm, zk, 1)):
        load = pltpu.make_async_copy(
            source, target.at[:, pl.ds(0, nx), :], in_sems.at[sem]
        )
        load.start()
        loads.append(load)
    barrier = pltpu.get_barrier_semaphore()
    near, relayed = row_groups(n_row)
    for offset in near:
        pl.semaphore_signal(
            barrier, inc=1, device_id={"row": flipped(row, offset, n_row)}, device_id_type=MESH
        )

    @pl.when(col < n_col - 1)
    def _():
        pl.semaphore_signal(barrier, inc=1, device_id={"col": col + 1}, device_id_type=MESH)

    @pl.when(col > 0)
    def _():
        pl.semaphore_signal(barrier, inc=1, device_id={"col": col - 1}, device_id_type=MESH)

    edge = jnp.zeros((nx, PAD, ny), jnp.float32)
    for buf in (xu, xk):
        buf[:, pl.ds(0, PAD), :] = edge
        buf[:, pl.ds(PAD + nz, PAD), :] = edge
    field = lambda x: xu[x, inner, :]
    cond = lambda x: xk[x, inner, :]

    @pl.when(col == 0)
    def _():
        pack_l[...] = jnp.zeros_like(pack_l)

    @pl.when(col == n_col - 1)
    def _():
        pack_r[...] = jnp.zeros_like(pack_r)

    lane = lax.broadcasted_iota(jnp.int32, (nz, ny), 1)
    pair = lane // 2
    packed = jnp.zeros((nz, ny), jnp.float32)
    pitch = nx + PITCH_PAD
    for source, target, load, base in ((zu, xu, loads[0], 0), (zk, xk, loads[1], nx)):
        load.wait()
        flat = source.reshape(nz * pitch, ny)
        for x in range(nx):
            value = flat[pl.ds(x, nz, stride=pitch), :]
            target[x, inner, :] = value
            packed = jnp.where(pair == base + x, pltpu.roll(value, 2 * (base + x) + 1, 1), packed)
    half = nz // 2
    pack[...] = jnp.where(
        lane[:half] < ny // 2, packed[:half], pltpu.roll(packed[half:], ny // 2, 1)
    )
    beside = jnp.minimum(col, 1) + jnp.minimum(n_col - 1 - col, 1)
    pl.semaphore_wait(barrier, len(near) + beside)

    to_right = pltpu.make_async_remote_copy(
        src_ref=pack, dst_ref=pack_l, send_sem=halo_send.at[0], recv_sem=halo_recv.at[0],
        device_id={"col": jnp.minimum(col + 1, n_col - 1)}, device_id_type=MESH,
    )
    to_left = pltpu.make_async_remote_copy(
        src_ref=pack, dst_ref=pack_r, send_sem=halo_send.at[1], recv_sem=halo_recv.at[1],
        device_id={"col": jnp.maximum(col - 1, 0)}, device_id_type=MESH,
    )

    @pl.when(col < n_col - 1)
    def _():
        to_right.start()

    @pl.when(col > 0)
    def _():
        to_left.start()

    if relayed:
        pl.semaphore_signal(
            row_token, inc=1, device_id={"row": flipped(row, 2, n_row)}, device_id_type=MESH
        )

    def pass_on(step):
        @pl.when(col < n_col - 1)
        def _():
            pl.semaphore_signal(
                col_token.at[0, step], inc=1, device_id={"col": col + 1}, device_id_type=MESH
            )

        @pl.when(col > 0)
        def _():
            pl.semaphore_signal(
                col_token.at[1, step], inc=1, device_id={"col": col - 1}, device_id_type=MESH
            )

    def take_in(step):
        @pl.when(col > 0)
        def _():
            pl.semaphore_wait(col_token.at[0, step], 1)

        @pl.when(col < n_col - 1)
        def _():
            pl.semaphore_wait(col_token.at[1, step], 1)

    if n_col > 2:
        pass_on(0)

    first_x = jnp.where(row == 0, 0.5, 0.0).astype(jnp.float32)
    last_x = jnp.where(row == n_row - 1, 0.5, 0.0).astype(jnp.float32)
    first_y = jnp.where(col == 0, 0.5, 0.0).astype(jnp.float32)
    last_y = jnp.where(col == n_col - 1, 0.5, 0.0).astype(jnp.float32)
    s = 1.0 + first_x * cond(0)
    prod = jnp.ones((nz, ny), jnp.float32)
    gff = jnp.zeros((nz, ny), jnp.float32)
    for x in range(nx):
        if x < nx - 1:
            e = 0.5 * (cond(x) + cond(x + 1))
            inv = 1.0 / (s + e)
            ratio = e * inv
            xr[x] = ratio
        else:
            inv = 1.0 / (s + last_x * cond(x))
        weight = prod * inv
        xinv[x] = inv
        xw[x] = weight
        gff = gff + prod * weight
        if x < nx - 1:
            prod = prod * ratio
            s = 1.0 + s * ratio
    for q, value in enumerate((gff, weight, inv, cond(0), cond(nx - 1))):
        for j in range(n_row):
            xm[j, q] = value[j * zs : (j + 1) * zs]
    if relayed:
        pl.semaphore_wait(row_token, 1)
    xm_copies = send_all("row", n_row, lambda peer: xm.at[peer], xm_in, xm_send, xm_recv)
    xm_in[row] = xm[row]

    below = first_x * cond(0) * field(0)
    for x in range(nx):
        u = field(x)
        k = cond(x)
        flux = 0.5 * (k + pltpu.roll(k, ny - 1, 1)) * (pltpu.roll(u, ny - 1, 1) - u)
        flux = jnp.where(lane == ny - 1, 0.0, flux)
        total = flux - pltpu.roll(flux, 1, 1)
        k_up, u_up = xk[x, pl.ds(PAD + 1, nz), :], xu[x, pl.ds(PAD + 1, nz), :]
        k_down, u_down = xk[x, pl.ds(PAD - 1, nz), :], xu[x, pl.ds(PAD - 1, nz), :]
        total = total + 0.5 * z_weight * ((k + k_up) * (u_up - u) - (k + k_down) * (u - u_down))
        if x < nx - 1:
            above = 0.5 * (k + cond(x + 1)) * (field(x + 1) - u)
        else:
            above = -last_x * k * u
        xb[x] = total + (above - below)
        below = above

    for p in range(blocks):
        per = LANES // nz
        tile = jnp.concatenate([cond(p * per + i) for i in range(per)], axis=0)
        kt[pl.ds(p, ny, stride=blocks), :] = tile.T

    @pl.when(col > 0)
    def _():
        to_right.wait_recv()

    @pl.when(col < n_col - 1)
    def _():
        to_left.wait_recv()

    for step in range(1, n_col - 2):
        take_in(step - 1)
        pass_on(step)
    small = lax.broadcasted_iota(jnp.int32, (nz // 2, ny), 1)
    other = jnp.where(
        small % 2 == 0, pltpu.roll(pack_r[...], ny - 1, 1), pltpu.roll(pack_l[...], 1, 1)
    )
    mine = pack[...]
    k_sum = pltpu.roll(mine + other, ny - 2 * nx, 1)
    outer = 0.5 * k_sum * (other - mine)
    ends = (lane == 0) | (lane == ny - 1)

    value = None
    for x in range(nx):
        place = ny - 1 - 2 * x
        outer_x = (pltpu.roll(outer, place, 1), pltpu.roll(outer, place - ny // 2, 1))
        here = xb[x] + jnp.where(ends, jnp.concatenate(outer_x, axis=0), 0.0)
        value = here if x == 0 else here + xr[x - 1] * value
        xb[x] = value
        free_first = xw[x] * value if x == 0 else free_first + xw[x] * value
    free_last = xinv[nx - 1] * value
    for q, v in enumerate((field(0) + free_first, field(nx - 1) + free_last)):
        for j in range(n_row):
            xv[j, q] = v[j * zs : (j + 1) * zs]
    xv_copies = send_all("row", n_row, lambda peer: xv.at[peer], xv_in, xv_send, xv_recv)
    xv_in[row] = xv[row]

    def y_at(y):
        if isinstance(y, int):
            return pl.ds(y * blocks, blocks)
        return pl.ds(pl.multiple_of(y * blocks, blocks), blocks)

    def y_factor(y, state):
        k, s, prod, gff = state
        k_next = kt[y_at(y + 1), :]
        e = 0.5 * (k + k_next)
        inv = 1.0 / (s + e)
        ratio = e * inv
        weight = prod * inv
        yr[y_at(y), :] = ratio
        yinv[y_at(y), :] = inv
        yw[y_at(y), :] = weight
        return k_next, 1.0 + s * ratio, prod * ratio, gff + prod * weight

    def unrolled(step, base, state):
        for i in range(UNROLL):
            state = step(base * UNROLL + i, state)
        return state

    trips = ny // UNROLL
    k_first = kt[y_at(0), :]
    one = jnp.ones_like(k_first)
    state = (k_first, 1.0 + first_y * k_first, one, jnp.zeros_like(one))
    state = lax.fori_loop(0, trips - 1, lambda t, c: unrolled(y_factor, t, c), state)
    for y in range((trips - 1) * UNROLL, ny - 1):
        state = y_factor(y, state)
    k_last, s, prod, gff = state
    inv = 1.0 / (s + last_y * k_last)
    weight = prod * inv
    gff = gff + prod * weight
    yinv[y_at(ny - 1), :] = inv
    yw[y_at(ny - 1), :] = weight
    for q, v in enumerate((gff, weight, inv, k_first, k_last)):
        ym[q] = v
    if n_col > 2:
        take_in(n_col - 3)
    ym_copies = send_all("col", n_col, lambda peer: ym, ym_in, ym_send, ym_recv)
    ym_in[col] = ym[...]

    for copy in xm_copies:
        copy.wait_recv()
    x_mats = lambda m, q: xm_in[m, q]
    x_rows = factor_faces(x_mats, n_row)
    for copy in xv_copies:
        copy.wait_recv()
    fluxes = solve_faces(x_rows, x_mats, lambda m, q: xv_in[m, q], n_row)
    nothing = jnp.zeros((zs, ny), jnp.float32)
    for m in range(n_row):
        xj[m, 0] = fluxes[m - 1] if m > 0 else nothing
        xj[m, 1] = fluxes[m] if m < n_row - 1 else nothing
    xj_copies = send_all("row", n_row, lambda peer: xj.at[peer], xj_in, xj_send, xj_recv)
    xj_in[row] = xj[row]

    for copy in ym_copies:
        copy.wait_recv()
    y_mats = lambda m, q: ym_in[m, q]
    y_rows = factor_faces(y_mats, n_col)
    for copy in xj_copies:
        copy.wait_recv()

    enter = jnp.concatenate([xj_in[j, 0] for j in range(n_row)], axis=0)
    leave = jnp.concatenate([xj_in[j, 1] for j in range(n_row)], axis=0)
    for x in reversed(range(nx)):
        if x == nx - 1:
            delta = (xb[x] + leave) * xinv[x] - enter * xw[x]
        else:
            delta = xb[x] * xinv[x] - enter * xw[x] + xr[x] * delta
        xb[x] = delta
    for p in range(blocks):
        tile = jnp.concatenate([xb[p * per + i] for i in range(per)], axis=0)
        dt[pl.ds(p, ny, stride=blocks), :] = tile.T

    def y_forward(y, state):
        value, free_first = state
        value = dt[y_at(y), :] + yr[y_at(y - 1), :] * value
        dt[y_at(y), :] = value
        return value, free_first + yw[y_at(y), :] * value

    value = dt[y_at(0), :]
    state = (value, yw[y_at(0), :] * value)
    for y in range(1, UNROLL):
        state = y_forward(y, state)
    value, free_first = lax.fori_loop(1, trips, lambda t, c: unrolled(y_forward, t, c), state)
    yv[0] = free_first
    yv[1] = yinv[y_at(ny - 1), :] * value
    yv_copies = send_all("col", n_col, lambda peer: yv, yv_in, yv_send, yv_recv)
    yv_in[col] = yv[...]
    for copy in yv_copies:
        copy.wait_recv()
    fluxes = solve_faces(y_rows, y_mats, lambda m, q: yv_in[m, q], n_col)
    enter = jnp.zeros_like(one)
    leave = jnp.zeros_like(one)
    for m in range(n_col - 1):
        enter = jnp.where(col == m + 1, fluxes[m], enter)
        leave = jnp.where(col == m, fluxes[m], leave)

    def y_backward(y, delta):
        free = dt[y_at(y), :] * yinv[y_at(y), :] - enter * yw[y_at(y), :]
        delta = free + yr[y_at(y), :] * delta
        dt[y_at(y), :] = delta
        return delta

    def y_backward_trip(t, delta):
        top = ny - 1 - t * UNROLL
        for i in range(UNROLL):
            delta = y_backward(top - i, delta)
        return delta

    delta = (value + leave) * yinv[y_at(ny - 1), :] - enter * yw[y_at(ny - 1), :]
    dt[y_at(ny - 1), :] = delta
    for y in reversed(range(ny - UNROLL, ny - 1)):
        delta = y_backward(y, delta)
    lax.fori_loop(1, trips, y_backward_trip, delta)
    for p in range(blocks):
        tile = dt[pl.ds(p, ny, stride=blocks), :].T
        for i in range(per):
            x = p * per + i
            out_ref[pl.ds(x, nz, stride=nx), :] = field(x) + tile[i * nz : (i + 1) * nz]

    @pl.when(col < n_col - 1)
    def _():
        to_right.wait_send()

    @pl.when(col > 0)
    def _():
        to_left.wait_send()

    for copies in (xm_copies, xv_copies, xj_copies, ym_copies, yv_copies):
        for copy in copies:
            copy.wait_send()


def solution(mesh):
    n_row, n_col = mesh.shape["row"], mesh.shape["col"]

    def on_device(field, conductivity):
        nz, nx, ny = field.shape
        zs = nz // n_row
        blocks = nz * nx // LANES
        flat = (nz * nx, ny)
        tall = pltpu.VMEM((nx, nz + 2 * PAD, ny), jnp.float32)
        wide = pltpu.VMEM((nz, nx + PITCH_PAD, ny), jnp.float32)
        cube = pltpu.VMEM((nx, nz, ny), jnp.float32)
        lines = pltpu.VMEM((ny * blocks, LANES), jnp.float32)
        plane = pltpu.VMEM((nz // 2, ny), jnp.float32)
        part = lambda count: pltpu.VMEM((n_row, count, zs, ny), jnp.float32)
        whole = lambda *lead: pltpu.VMEM((*lead, blocks, LANES), jnp.float32)
        sems = lambda count: pltpu.SemaphoreType.DMA((count,))
        out = pl.pallas_call(
            functools.partial(kernel, (n_row, n_col, nz, nx, ny)),
            out_shape=jax.ShapeDtypeStruct(flat, jnp.float32),
            in_specs=[pl.BlockSpec(memory_space=pltpu.HBM)] * 2,
            out_specs=pl.BlockSpec(memory_space=pltpu.VMEM),
            scratch_shapes=[
                wide, wide, tall, tall, cube, cube, cube, cube,
                lines, lines, lines, lines, lines,
                plane, plane, plane,
                part(5), part(5), part(2), part(2), part(2), part(2),
                whole(n_col, 5), whole(n_col, 2), whole(5), whole(2),
                sems(2), sems(2), sems(2),
                *[sems(n_row)] * 6,
                *[sems(n_col)] * 4,
                pltpu.SemaphoreType.REGULAR,
                pltpu.SemaphoreType.REGULAR((2, n_col)),
            ],
            compiler_params=pltpu.CompilerParams(
                collective_id=0, has_side_effects=True, vmem_limit_bytes=32 * 1024 * 1024
            ),
            name="adi_step",
        )(
            pltpu.with_memory_space_constraint(field, pltpu.HBM),
            pltpu.with_memory_space_constraint(conductivity, pltpu.HBM),
        )
        return out.reshape(field.shape)

    spec = P(None, "row", "col")
    return jax.shard_map(
        on_device, mesh=mesh, in_specs=(spec, spec), out_specs=spec, check_vma=False
    )
```

```python
import functools

import jax
import jax.numpy as jnp
from jax import lax
from jax.experimental import pallas as pl
from jax.experimental.pallas import tpu as pltpu
from jax.sharding import PartitionSpec as P

MESH = pl.DeviceIdType.MESH
z_weight = 0.02
LANES = 128
UNROLL = 8
PAD = 8
PITCH_PAD = 8


def row_groups(count):
    every = range(1, count)
    if count < 8 or count & (count - 1):
        return list(every), False
    return [o for o in every if not (o & 2 and o >> 2)], True


def flipped(index, offset, count):
    if count & (count - 1):
        return lax.rem(index + offset, count)
    result = index
    bit = 1
    while bit <= offset:
        if offset & bit:
            result = result + bit * (1 - 2 * ((index // bit) % 2))
        bit *= 2
    return result


def send_all(axis, count, source_of, target, send_sems, recv_sems, offsets=None):
    me = lax.axis_index(axis)
    copies = []
    for offset in offsets or range(count - 1, 0, -1):
        peer = flipped(me, offset, count)
        copy = pltpu.make_async_remote_copy(
            src_ref=source_of(peer),
            dst_ref=target.at[me],
            send_sem=send_sems.at[offset],
            recv_sem=recv_sems.at[offset],
            device_id={axis: peer},
            device_id_type=MESH,
        )
        copy.start()
        copies.append(copy)
    return copies


def factor_faces(mats, count):
    rows = []
    h_prev = None
    for m in range(count - 1):
        face = 0.5 * (mats(m, 4) + mats(m + 1, 3))
        pivot = 1.0 / face + mats(m + 1, 0) + mats(m, 2)
        if m > 0:
            pivot = pivot - mats(m, 1) * h_prev
        inverse = 1.0 / pivot
        h_prev = mats(m + 1, 1) * inverse
        rows.append((inverse, h_prev))
    return rows


def solve_faces(rows, mats, values, count):
    partial = []
    for m in range(count - 1):
        right = values(m + 1, 0) - values(m, 1)
        if m > 0:
            right = right + mats(m, 1) * partial[-1]
        partial.append(right * rows[m][0])
    fluxes = [None] * (count - 1)
    for m in reversed(range(count - 1)):
        fluxes[m] = partial[m]
        if m < count - 2:
            fluxes[m] = fluxes[m] + rows[m][1] * fluxes[m + 1]
    return fluxes


def kernel(
    dims, field_hbm, cond_hbm, out_ref,
    zu, zk, xu, xk, xr, xinv, xw, xb, kt, yr, yinv, yw, dt,
    pack, pack_l, pack_r, xm, xm_in, xv, xv_in, xj, xj_in, ym_in, yv_in, ym, yv,
    in_sems, halo_send, halo_recv, xm_send, xm_recv, xv_send, xv_recv, xj_send, xj_recv,
    ym_send, ym_recv, yv_send, yv_recv, row_token, col_token,
):
    n_row, n_col, nz, nx, ny = dims
    zs = nz // n_row
    blocks = nz * nx // LANES
    row = lax.axis_index("row")
    col = lax.axis_index("col")
    inner = pl.ds(PAD, nz)
    loads = []
    for source, target, sem in ((field_hbm, zu, 0), (cond_hbm, zk, 1)):
        load = pltpu.make_async_copy(
            source, target.at[:, pl.ds(0, nx), :], in_sems.at[sem]
        )
        load.start()
        loads.append(load)
    barrier = pltpu.get_barrier_semaphore()
    near, relayed = row_groups(n_row)
    for offset in near:
        pl.semaphore_signal(
            barrier, inc=1, device_id={"row": flipped(row, offset, n_row)}, device_id_type=MESH
        )

    @pl.when(col < n_col - 1)
    def _():
        pl.semaphore_signal(barrier, inc=1, device_id={"col": col + 1}, device_id_type=MESH)

    @pl.when(col > 0)
    def _():
        pl.semaphore_signal(barrier, inc=1, device_id={"col": col - 1}, device_id_type=MESH)

    edge = jnp.zeros((nx, PAD, ny), jnp.float32)
    for buf in (xu, xk):
        buf[:, pl.ds(0, PAD), :] = edge
        buf[:, pl.ds(PAD + nz, PAD), :] = edge
    field = lambda x: xu[x, inner, :]
    cond = lambda x: xk[x, inner, :]

    @pl.when(col == 0)
    def _():
        pack_l[...] = jnp.zeros_like(pack_l)

    @pl.when(col == n_col - 1)
    def _():
        pack_r[...] = jnp.zeros_like(pack_r)

    lane = lax.broadcasted_iota(jnp.int32, (nz, ny), 1)
    pair = lane // 2
    packed = jnp.zeros((nz, ny), jnp.float32)
    pitch = nx + PITCH_PAD
    for source, target, load, base in ((zu, xu, loads[0], 0), (zk, xk, loads[1], nx)):
        load.wait()
        flat = source.reshape(nz * pitch, ny)
        for x in range(nx):
            value = flat[pl.ds(x, nz, stride=pitch), :]
            target[x, inner, :] = value
            packed = jnp.where(pair == base + x, pltpu.roll(value, 2 * (base + x) + 1, 1), packed)
    half = nz // 2
    pack[...] = jnp.where(
        lane[:half] < ny // 2, packed[:half], pltpu.roll(packed[half:], ny // 2, 1)
    )
    first_x = jnp.where(row == 0, 0.5, 0.0).astype(jnp.float32)
    last_x = jnp.where(row == n_row - 1, 0.5, 0.0).astype(jnp.float32)
    first_y = jnp.where(col == 0, 0.5, 0.0).astype(jnp.float32)
    last_y = jnp.where(col == n_col - 1, 0.5, 0.0).astype(jnp.float32)
    s = 1.0 + first_x * cond(0)
    prod = jnp.ones((nz, ny), jnp.float32)
    gff = jnp.zeros((nz, ny), jnp.float32)
    for x in range(nx):
        if x < nx - 1:
            e = 0.5 * (cond(x) + cond(x + 1))
            inv = 1.0 / (s + e)
            ratio = e * inv
            xr[x] = ratio
        else:
            inv = 1.0 / (s + last_x * cond(x))
        weight = prod * inv
        xinv[x] = inv
        xw[x] = weight
        gff = gff + prod * weight
        if x < nx - 1:
            prod = prod * ratio
            s = 1.0 + s * ratio
    for q, value in enumerate((gff, weight, inv, cond(0), cond(nx - 1))):
        for j in range(n_row):
            xm[j, q] = value[j * zs : (j + 1) * zs]
    below = first_x * cond(0) * field(0)
    for x in range(nx):
        u = field(x)
        k = cond(x)
        flux = 0.5 * (k + pltpu.roll(k, ny - 1, 1)) * (pltpu.roll(u, ny - 1, 1) - u)
        flux = jnp.where(lane == ny - 1, 0.0, flux)
        total = flux - pltpu.roll(flux, 1, 1)
        k_up, u_up = xk[x, pl.ds(PAD + 1, nz), :], xu[x, pl.ds(PAD + 1, nz), :]
        k_down, u_down = xk[x, pl.ds(PAD - 1, nz), :], xu[x, pl.ds(PAD - 1, nz), :]
        total = total + 0.5 * z_weight * ((k + k_up) * (u_up - u) - (k + k_down) * (u - u_down))
        if x < nx - 1:
            above = 0.5 * (k + cond(x + 1)) * (field(x + 1) - u)
        else:
            above = -last_x * k * u
        xb[x] = total + (above - below)
        below = above

    beside = jnp.minimum(col, 1) + jnp.minimum(n_col - 1 - col, 1)
    pl.semaphore_wait(barrier, len(near) + beside)

    to_right = pltpu.make_async_remote_copy(
        src_ref=pack, dst_ref=pack_l, send_sem=halo_send.at[0], recv_sem=halo_recv.at[0],
        device_id={"col": jnp.minimum(col + 1, n_col - 1)}, device_id_type=MESH,
    )
    to_left = pltpu.make_async_remote_copy(
        src_ref=pack, dst_ref=pack_r, send_sem=halo_send.at[1], recv_sem=halo_recv.at[1],
        device_id={"col": jnp.maximum(col - 1, 0)}, device_id_type=MESH,
    )

    @pl.when(col < n_col - 1)
    def _():
        to_right.start()

    @pl.when(col > 0)
    def _():
        to_left.start()

    if relayed:
        pl.semaphore_signal(
            row_token, inc=1, device_id={"row": flipped(row, 2, n_row)}, device_id_type=MESH
        )

    def pass_on(step):
        @pl.when(col < n_col - 1)
        def _():
            pl.semaphore_signal(
                col_token.at[0, step], inc=1, device_id={"col": col + 1}, device_id_type=MESH
            )

        @pl.when(col > 0)
        def _():
            pl.semaphore_signal(
                col_token.at[1, step], inc=1, device_id={"col": col - 1}, device_id_type=MESH
            )

    def take_in(step):
        @pl.when(col > 0)
        def _():
            pl.semaphore_wait(col_token.at[0, step], 1)

        @pl.when(col < n_col - 1)
        def _():
            pl.semaphore_wait(col_token.at[1, step], 1)

    if n_col > 2:
        pass_on(0)

    xm_from = lambda peer: xm.at[peer]
    xm_copies = send_all("row", n_row, xm_from, xm_in, xm_send, xm_recv, near)
    xm_in[row] = xm[row]

    for p in range(blocks):
        per = LANES // nz
        tile = jnp.concatenate([cond(p * per + i) for i in range(per)], axis=0)
        kt[pl.ds(p, ny, stride=blocks), :] = tile.T

    if relayed:
        pl.semaphore_wait(row_token, 1)
        far = [o for o in range(1, n_row) if o not in near]
        xm_copies = xm_copies + send_all("row", n_row, xm_from, xm_in, xm_send, xm_recv, far)
    for step in range(1, n_col - 2):
        take_in(step - 1)
        pass_on(step)

    def y_at(y):
        if isinstance(y, int):
            return pl.ds(y * blocks, blocks)
        return pl.ds(pl.multiple_of(y * blocks, blocks), blocks)

    def y_factor(y, state):
        k, s, prod, gff = state
        k_next = kt[y_at(y + 1), :]
        e = 0.5 * (k + k_next)
        inv = 1.0 / (s + e)
        ratio = e * inv
        weight = prod * inv
        yr[y_at(y), :] = ratio
        yinv[y_at(y), :] = inv
        yw[y_at(y), :] = weight
        return k_next, 1.0 + s * ratio, prod * ratio, gff + prod * weight

    def unrolled(step, base, state):
        for i in range(UNROLL):
            state = step(base * UNROLL + i, state)
        return state

    trips = ny // UNROLL
    k_first = kt[y_at(0), :]
    one = jnp.ones_like(k_first)
    state = (k_first, 1.0 + first_y * k_first, one, jnp.zeros_like(one))
    state = lax.fori_loop(0, trips - 1, lambda t, c: unrolled(y_factor, t, c), state)
    for y in range((trips - 1) * UNROLL, ny - 1):
        state = y_factor(y, state)
    k_last, s, prod, gff = state
    inv = 1.0 / (s + last_y * k_last)
    weight = prod * inv
    gff = gff + prod * weight
    yinv[y_at(ny - 1), :] = inv
    yw[y_at(ny - 1), :] = weight
    for q, v in enumerate((gff, weight, inv, k_first, k_last)):
        ym[q] = v
    if n_col > 2:
        take_in(n_col - 3)
    ym_copies = send_all("col", n_col, lambda peer: ym, ym_in, ym_send, ym_recv)
    ym_in[col] = ym[...]

    @pl.when(col > 0)
    def _():
        to_right.wait_recv()

    @pl.when(col < n_col - 1)
    def _():
        to_left.wait_recv()

    small = lax.broadcasted_iota(jnp.int32, (nz // 2, ny), 1)
    other = jnp.where(
        small % 2 == 0, pltpu.roll(pack_r[...], ny - 1, 1), pltpu.roll(pack_l[...], 1, 1)
    )
    mine = pack[...]
    k_sum = pltpu.roll(mine + other, ny - 2 * nx, 1)
    outer = 0.5 * k_sum * (other - mine)
    ends = (lane == 0) | (lane == ny - 1)

    value = None
    for x in range(nx):
        place = ny - 1 - 2 * x
        outer_x = (pltpu.roll(outer, place, 1), pltpu.roll(outer, place - ny // 2, 1))
        here = xb[x] + jnp.where(ends, jnp.concatenate(outer_x, axis=0), 0.0)
        value = here if x == 0 else here + xr[x - 1] * value
        xb[x] = value
        free_first = xw[x] * value if x == 0 else free_first + xw[x] * value
    free_last = xinv[nx - 1] * value
    for q, v in enumerate((field(0) + free_first, field(nx - 1) + free_last)):
        for j in range(n_row):
            xv[j, q] = v[j * zs : (j + 1) * zs]
    xv_copies = send_all("row", n_row, lambda peer: xv.at[peer], xv_in, xv_send, xv_recv)
    xv_in[row] = xv[row]

    for copy in xm_copies:
        copy.wait_recv()
    x_mats = lambda m, q: xm_in[m, q]
    x_rows = factor_faces(x_mats, n_row)
    for copy in xv_copies:
        copy.wait_recv()
    fluxes = solve_faces(x_rows, x_mats, lambda m, q: xv_in[m, q], n_row)
    nothing = jnp.zeros((zs, ny), jnp.float32)
    for m in range(n_row):
        xj[m, 0] = fluxes[m - 1] if m > 0 else nothing
        xj[m, 1] = fluxes[m] if m < n_row - 1 else nothing
    xj_copies = send_all("row", n_row, lambda peer: xj.at[peer], xj_in, xj_send, xj_recv)
    xj_in[row] = xj[row]

    for copy in ym_copies:
        copy.wait_recv()
    y_mats = lambda m, q: ym_in[m, q]
    y_rows = factor_faces(y_mats, n_col)
    for copy in xj_copies:
        copy.wait_recv()

    enter = jnp.concatenate([xj_in[j, 0] for j in range(n_row)], axis=0)
    leave = jnp.concatenate([xj_in[j, 1] for j in range(n_row)], axis=0)
    for x in reversed(range(nx)):
        if x == nx - 1:
            delta = (xb[x] + leave) * xinv[x] - enter * xw[x]
        else:
            delta = xb[x] * xinv[x] - enter * xw[x] + xr[x] * delta
        xb[x] = delta
    for p in range(blocks):
        tile = jnp.concatenate([xb[p * per + i] for i in range(per)], axis=0)
        dt[pl.ds(p, ny, stride=blocks), :] = tile.T

    def y_forward(y, state):
        value, free_first = state
        value = dt[y_at(y), :] + yr[y_at(y - 1), :] * value
        dt[y_at(y), :] = value
        return value, free_first + yw[y_at(y), :] * value

    value = dt[y_at(0), :]
    state = (value, yw[y_at(0), :] * value)
    for y in range(1, UNROLL):
        state = y_forward(y, state)
    value, free_first = lax.fori_loop(1, trips, lambda t, c: unrolled(y_forward, t, c), state)
    yv[0] = free_first
    yv[1] = yinv[y_at(ny - 1), :] * value
    yv_copies = send_all("col", n_col, lambda peer: yv, yv_in, yv_send, yv_recv)
    yv_in[col] = yv[...]
    for copy in yv_copies:
        copy.wait_recv()
    fluxes = solve_faces(y_rows, y_mats, lambda m, q: yv_in[m, q], n_col)
    enter = jnp.zeros_like(one)
    leave = jnp.zeros_like(one)
    for m in range(n_col - 1):
        enter = jnp.where(col == m + 1, fluxes[m], enter)
        leave = jnp.where(col == m, fluxes[m], leave)

    def y_backward(y, delta):
        free = dt[y_at(y), :] * yinv[y_at(y), :] - enter * yw[y_at(y), :]
        delta = free + yr[y_at(y), :] * delta
        dt[y_at(y), :] = delta
        return delta

    def y_backward_trip(t, delta):
        top = ny - 1 - t * UNROLL
        for i in range(UNROLL):
            delta = y_backward(top - i, delta)
        return delta

    delta = (value + leave) * yinv[y_at(ny - 1), :] - enter * yw[y_at(ny - 1), :]
    dt[y_at(ny - 1), :] = delta
    for y in reversed(range(ny - UNROLL, ny - 1)):
        delta = y_backward(y, delta)
    lax.fori_loop(1, trips, y_backward_trip, delta)
    for p in range(blocks):
        tile = dt[pl.ds(p, ny, stride=blocks), :].T
        for i in range(per):
            x = p * per + i
            out_ref[pl.ds(x, nz, stride=nx), :] = field(x) + tile[i * nz : (i + 1) * nz]

    @pl.when(col < n_col - 1)
    def _():
        to_right.wait_send()

    @pl.when(col > 0)
    def _():
        to_left.wait_send()

    for copies in (xm_copies, xv_copies, xj_copies, ym_copies, yv_copies):
        for copy in copies:
            copy.wait_send()


def solution(mesh):
    n_row, n_col = mesh.shape["row"], mesh.shape["col"]

    def on_device(field, conductivity):
        nz, nx, ny = field.shape
        zs = nz // n_row
        blocks = nz * nx // LANES
        flat = (nz * nx, ny)
        tall = pltpu.VMEM((nx, nz + 2 * PAD, ny), jnp.float32)
        wide = pltpu.VMEM((nz, nx + PITCH_PAD, ny), jnp.float32)
        cube = pltpu.VMEM((nx, nz, ny), jnp.float32)
        lines = pltpu.VMEM((ny * blocks, LANES), jnp.float32)
        plane = pltpu.VMEM((nz // 2, ny), jnp.float32)
        part = lambda count: pltpu.VMEM((n_row, count, zs, ny), jnp.float32)
        whole = lambda *lead: pltpu.VMEM((*lead, blocks, LANES), jnp.float32)
        sems = lambda count: pltpu.SemaphoreType.DMA((count,))
        out = pl.pallas_call(
            functools.partial(kernel, (n_row, n_col, nz, nx, ny)),
            out_shape=jax.ShapeDtypeStruct(flat, jnp.float32),
            in_specs=[pl.BlockSpec(memory_space=pltpu.HBM)] * 2,
            out_specs=pl.BlockSpec(memory_space=pltpu.VMEM),
            scratch_shapes=[
                wide, wide, tall, tall, cube, cube, cube, cube,
                lines, lines, lines, lines, lines,
                plane, plane, plane,
                part(5), part(5), part(2), part(2), part(2), part(2),
                whole(n_col, 5), whole(n_col, 2), whole(5), whole(2),
                sems(2), sems(2), sems(2),
                *[sems(n_row)] * 6,
                *[sems(n_col)] * 4,
                pltpu.SemaphoreType.REGULAR,
                pltpu.SemaphoreType.REGULAR((2, n_col)),
            ],
            compiler_params=pltpu.CompilerParams(
                collective_id=0, has_side_effects=True, vmem_limit_bytes=32 * 1024 * 1024
            ),
            name="adi_step",
        )(
            pltpu.with_memory_space_constraint(field, pltpu.HBM),
            pltpu.with_memory_space_constraint(conductivity, pltpu.HBM),
        )
        return out.reshape(field.shape)

    spec = P(None, "row", "col")
    return jax.shard_map(
        on_device, mesh=mesh, in_specs=(spec, spec), out_specs=spec, check_vma=False
    )
```
